32 devices in a mesh: grp: 2 (over x), req: 16 (over z, y, core).
Axes of the slice: x: 2, y: 2, z: 4, core: 2. Of those that a mesh axis runs over, the one named last changes fastest.
Arguments:
- moe_input: bfloat16 [512, 2048], P(('grp', 'req')), parts along dimension 0, may hold values from -6 to 6
- norm_gain: bfloat16 [2048], replicated, may hold values from 0.25 to 1.75
- route_ids: int32 [512, 8], P(('grp', 'req')), parts along dimension 0, may hold values from 0 to 15, all different within a row; in each aligned block of 16 rows (0 to 15, 16 to 31, ...) at most 16 rows name the same one
- route_gates: bfloat16 [512, 8], P(('grp', 'req')), parts along dimension 0, may hold values from 0.049804688 to 0.5
- expert_gate: bfloat16 [16, 2048, 768], P('req'), may hold values from -0.125 to 0.125
- expert_up: bfloat16 [16, 2048, 768], P('req'), may hold values from -0.125 to 0.125
- expert_down: bfloat16 [16, 768, 2048], P('req'), may hold values from -0.21875 to 0.21875
- queries: bfloat16 [128, 4096], P(('grp', 'req')), parts along dimension 0, may hold values from -4.5 to 4.5
- keys_cache: bfloat16 [128, 4, 384, 128], P(('grp', 'req')), parts along dimension 0, may hold values from -4.5 to 4.5
- values_cache: bfloat16 [128, 4, 384, 128], P(('grp', 'req')), parts along dimension 0, may hold values from -4.5 to 4.5
- new_keys: bfloat16 [128, 512], P(('grp', 'req')), parts along dimension 0, may hold values from -4.5 to 4.5
- new_values: bfloat16 [128, 512], P(('grp', 'req')), parts along dimension 0, may hold values from -4.5 to 4.5
- cache_lengths: int32 [128], P(('grp', 'req')), parts along dimension 0, may hold values from 1 to 384
Outputs:
- moe_out: bfloat16 [512, 2048], P(('grp', 'req')), parts along dimension 0
- attention_out: bfloat16 [128, 4096], P(('grp', 'req')), parts along dimension 0
The draws below stay inside these ranges and needn't reach their ends.
There are 2 independent parts, one for each index of `grp`. The reference program is written for one: setup_inputs(seed, part) draws one part's arguments, and reference() takes and returns one part's arrays. A program takes and returns all parts, laid end to end along the dimension named above; an argument that names none is the same for every part. Nothing has to cross between parts.
Inputs may be any that keep to these rules, and one draw needn't show every extreme that they name: `route_ids`: each row names 8 different experts; in each aligned block of 16 rows (the rows of one device) no expert is named by more than 16 rows, a bound that some block reaches.
All inputs are finite; a program needn't handle non-finite values.
Results may differ from the reference program's by a relative error of at most 0.0065.
Values may be sent and summed in bfloat16 or wider, within the bound.
No kernel may reach another device: no remote copies, remote signals or barrier semaphores. Data moves between devices by JAX's collectives and lax.ppermute only.
A program may use at most 64 MiB of HBM per device.

```python
import math
import jax
import jax.numpy as jnp
import numpy as np
from jax import lax

D = 2048
FF = 768
QH = 32
KVH = 4
HD = 128
TOP = 8
L_MAX = 384
R_DEV = 16
EXPERTS = 16
CAP = 16
QPK = 8
ROWS = 256
ROWS_B = 64
N_REQ = 16


def attention_draw(key):
    query_key = jax.random.fold_in(key, 11)
    cache_key = jax.random.fold_in(key, 12)
    fresh_key = jax.random.fold_in(key, 13)
    queries = jax.random.truncated_normal(query_key, -4.5, 4.5, (ROWS_B, QH * HD), jnp.float32)
    cached = jax.random.truncated_normal(cache_key, -4.5, 4.5, (ROWS_B, KVH, L_MAX, HD), jnp.float32)
    fresh = jax.random.truncated_normal(fresh_key, -4.5, 4.5, (ROWS_B, KVH * HD), jnp.float32)
    return (queries, cached, fresh)


def draw_queries(key, part):
    return attention_draw(key)[0].astype(jnp.bfloat16)


def draw_keys_cache(key, part):
    return attention_draw(key)[1].astype(jnp.bfloat16)


def draw_new_keys(key, part):
    return attention_draw(key)[2].astype(jnp.bfloat16)


def plant(entries, own_key, least, top_value):
    longest = entries.shape.index(max(entries.shape))
    spots = []
    for shift in (0, 1):
        where = [jax.random.randint(jax.random.fold_in(own_key, axis), (), 0, length) for axis, length in enumerate(entries.shape)]
        where[longest] = (where[longest] + shift) % entries.shape[longest]
        spots.append(tuple(where))
    return entries.at[spots[0]].set(least).at[spots[1]].set(top_value)


def block_levels(own_key, shape, pieces, least, largest):
    gain = 1.0
    for axis_at, parts in pieces:
        draws = jax.random.uniform(jax.random.fold_in(jax.random.fold_in(own_key, 6), axis_at), (parts,), jnp.float32, least / len(pieces), largest / len(pieces))
        gain = gain * jnp.repeat(jnp.exp(draws), shape[axis_at] // parts).reshape((-1,) + (1,) * (len(shape) - 1 - axis_at))
    return gain


def deal_out(key, own, number, rows, amount, top, limit, lean):
    order = jax.random.permutation(key, amount)
    crowded, usual = load_shares(amount, rows * top, limit, lean, True), load_shares(amount, rows * top, limit, lean, False)
    places = jnp.arange(amount)

    def named(sizes, turn):
        used = int((sizes > 0).sum())
        fixed = max(1, used // 4)
        shifted = fixed + (places - fixed + turn * (used - fixed)) % max(1, amount - fixed)
        return jnp.zeros((amount,), jnp.int32).at[order[jnp.where(places < fixed, places, shifted)]].set(jnp.asarray(sizes, jnp.int32))

    sizes = jnp.where(number % 4 == 0, named(crowded, number // 4), named(usual, number - number // 4 - 1))
    mixed = jax.random.permutation(jax.random.fold_in(own, 3), amount)
    giver, sink = mixed[0:amount // 2 * 2:2], mixed[1:amount // 2 * 2:2]
    margin = jnp.minimum(sizes[giver] - 1, limit - sizes[sink]) // 2
    margin = jnp.where((giver == order[0]) | (sink == order[0]) | (sizes[sink] == 0), 0, jnp.maximum(margin, 0))
    shifted = jax.random.randint(jax.random.fold_in(own, 4), (amount // 2,), 0, 1 << 20) % (margin + 1)
    sizes = sizes.at[giver].add(-shifted).at[sink].add(shifted)
    members = jnp.searchsorted(jnp.cumsum(sizes), jnp.arange(rows * top), side="right").astype(jnp.int32)
    table = members.reshape(top, rows).T
    table = table[jax.random.permutation(jax.random.fold_in(own, 1), rows)]
    turn = jax.random.randint(jax.random.fold_in(own, 2), (rows, 1), 0, top)
    return jnp.take_along_axis(table, (jnp.arange(top)[None, :] + turn) % top, axis=1)


def load_shares(number_of, total, bound, slope, full):
    weights = [(1 << 20) // math.isqrt(rank ** slope) + 1 for rank in range(1, number_of + 1)]
    largest = bound if full else min(bound, max(-(-total // number_of), total * weights[0] // sum(weights)))
    least = 1 if total - largest >= number_of - 1 else 0
    given, surplus = [largest] + [least] * (number_of - 1), total - largest - least * (number_of - 1)
    while surplus > 0:
        movable = [i for i in range(1, number_of) if given[i] < largest] or [i for i in range(1, number_of) if given[i] < bound]
        whole, remaining = sum([weights[i] for i in movable]), surplus
        for i in movable:
            more = min(bound - given[i], max(1, remaining * weights[i] // whole), surplus)
            given[i] = given[i] + more
            surplus = surplus - more
    return np.array(given)


def bell_draw(own_key, extent, spread, reach, shards=(), held_as=jnp.bfloat16):
    values = jax.random.normal(own_key, extent, jnp.float32) * spread
    if len(shards) > 0:
        values = block_levels(own_key, extent, shards, -0.22, 0.18) * values
    return jnp.clip(values, min=-reach, max=reach).astype(held_as)


def setup_inputs(seed: int = 0, part: int = 0) -> dict:
    key_list = jax.random.split(jax.random.key(seed), 14)
    part_keys = jax.random.split(jax.random.fold_in(key_list[13], part), 14)
    moe_input = bell_draw(part_keys[0], (ROWS, D), 1.0, 6.0, ((0, 16),))
    norm_gain = jnp.clip(1.0 + 0.15 * jax.random.normal(key_list[1], (D,), jnp.float32), 0.25, 1.75).astype(jnp.bfloat16)
    route_ids_keys = jax.random.split(jax.random.fold_in(part_keys[2], 1), ROWS // R_DEV)
    route_ids_turns = jax.random.permutation(jax.random.fold_in(part_keys[2], 3), ROWS // R_DEV)
    route_ids = jax.vmap(lambda own, number: deal_out(jax.random.fold_in(part_keys[2], 2), own, number, R_DEV, EXPERTS, TOP, CAP, 2))(route_ids_keys, route_ids_turns).reshape((ROWS, TOP))
    route_gates = jnp.clip(0.049804688 + 0.4501953 * jax.random.uniform(part_keys[3], (ROWS, TOP), jnp.float32) ** block_levels(part_keys[3], (ROWS, TOP), ((0, 16),), -0.2, 0.2), 0.049804688, 0.5).astype(jnp.bfloat16)
    expert_gate = bell_draw(key_list[4], (EXPERTS, D, FF), D ** -0.5, 0.125, ((0, 16),))
    expert_up = bell_draw(key_list[5], (EXPERTS, D, FF), D ** -0.5, 0.125, ((0, 16),))
    expert_down = bell_draw(key_list[6], (EXPERTS, FF, D), FF ** -0.5, 0.21875, ((0, 16),))
    queries = draw_queries(jax.random.fold_in(jax.random.fold_in(key_list[13], part), 71), part)
    keys_cache = draw_keys_cache(jax.random.fold_in(jax.random.fold_in(key_list[13], part), 71), part)
    values_cache = bell_draw(part_keys[9], (ROWS_B, KVH, L_MAX, HD), 1.0, 4.5, ((0, 16),))
    new_keys = draw_new_keys(jax.random.fold_in(jax.random.fold_in(key_list[13], part), 71), part)
    new_values = bell_draw(part_keys[11], (ROWS_B, KVH * HD), 1.0, 4.5, ((0, 16),))
    cache_lengths = plant(jax.random.randint(part_keys[12], (ROWS_B,), 1, L_MAX + 1), jax.random.fold_in(part_keys[12], 1), 1, L_MAX).astype(jnp.int32)
    return dict(moe_input=moe_input, norm_gain=norm_gain, route_ids=route_ids, route_gates=route_gates, expert_gate=expert_gate, expert_up=expert_up, expert_down=expert_down, queries=queries, keys_cache=keys_cache, values_cache=values_cache, new_keys=new_keys, new_values=new_values, cache_lengths=cache_lengths)


EPS = 1e-06

def slot_table(route_ids, experts, capacity):
    onehot = (route_ids[:, :, None] == jnp.arange(experts, dtype=jnp.int32)[None, None, :]).astype(jnp.float32)
    present = lax.optimization_barrier(jnp.sum(onehot, axis=1))
    earlier = jnp.cumsum(present, axis=0) - present
    levels = jnp.arange(capacity, dtype=jnp.float32)
    placed = present[:, :, None] * (earlier[:, :, None] == levels[None, None, :]).astype(jnp.float32)
    return (onehot, placed)

def expert_rows(packed):
    w_gate, w_up, w_down, received = packed
    flat = received.reshape(-1, D)
    gate_part = jnp.dot(flat, w_gate, preferred_element_type=jnp.float32)
    up_part = jnp.dot(flat, w_up, preferred_element_type=jnp.float32)
    active = (jax.nn.silu(gate_part) * up_part).astype(jnp.bfloat16)
    produced = jnp.dot(active, w_down, preferred_element_type=jnp.float32).astype(jnp.bfloat16)
    return produced.reshape(received.shape)

def attend(queries, keys_cache, values_cache, new_keys, new_values, cache_lengths):
    batch_rows = queries.shape[0]
    score_scale = HD ** (-0.5)
    grouped = queries.astype(jnp.float32).reshape(batch_rows, KVH, QPK, HD)
    scores = jnp.einsum('bgqd,bgld->bgql', grouped, keys_cache.astype(jnp.float32)) * score_scale
    own_score = jnp.einsum('bgqd,bgd->bgq', grouped, new_keys.astype(jnp.float32).reshape(batch_rows, KVH, HD)) * score_scale
    live_mask = (jnp.arange(L_MAX, dtype=jnp.int32)[None, :] < cache_lengths[:, None])[:, None, None, :]
    highest = jnp.maximum(lax.optimization_barrier(jnp.max(jnp.where(live_mask, scores, -jnp.inf), axis=-1)), own_score)
    weights = jnp.where(live_mask, jnp.exp(scores - highest[..., None]), 0.0)
    own_weight = jnp.exp(own_score - highest)
    totals = lax.optimization_barrier(jnp.sum(weights, axis=-1)) + own_weight
    prob_low = (weights / totals[..., None]).astype(jnp.bfloat16)
    own_prob = (own_weight / totals).astype(jnp.bfloat16)
    mixed_out = jnp.einsum('bgql,bgld->bgqd', prob_low.astype(jnp.float32), values_cache.astype(jnp.float32))
    mixed_out = mixed_out + own_prob.astype(jnp.float32)[..., None] * new_values.astype(jnp.float32).reshape(batch_rows, KVH, 1, HD)
    return mixed_out.reshape(batch_rows, QH * HD).astype(jnp.bfloat16)

def reference(moe_input, norm_gain, route_ids, route_gates, expert_gate, expert_up, expert_down, queries, keys_cache, values_cache, new_keys, new_values, cache_lengths):
    hidden = moe_input.astype(jnp.float32)
    normed = (hidden * lax.rsqrt(lax.optimization_barrier(jnp.mean(hidden * hidden, axis=-1, keepdims=True)) + EPS) * norm_gain.astype(jnp.float32)).astype(jnp.bfloat16)
    blocks = normed.reshape(N_REQ, R_DEV, D)
    id_blocks = route_ids.reshape(N_REQ, R_DEV, TOP)
    onehot, placed = jax.vmap(lambda block_ids: slot_table(block_ids, EXPERTS, CAP))(id_blocks)
    sent = jnp.einsum('nrec,nrd->necd', placed, blocks.astype(jnp.float32)).astype(jnp.bfloat16)
    produced = lax.map(expert_rows, (expert_gate, expert_up, expert_down, jnp.swapaxes(sent, 0, 1)))
    returned = jnp.swapaxes(produced, 0, 1)
    gate_blocks = route_gates.astype(jnp.float32).reshape(N_REQ, R_DEV, TOP)
    weight = jnp.einsum('nrke,nrk->nre', onehot, gate_blocks)
    combine = weight[..., None] * placed
    expert_sum = jnp.einsum('nrec,necd->nrd', combine, returned.astype(jnp.float32))
    moe_out = (hidden + expert_sum.reshape(ROWS, D)).astype(jnp.bfloat16)
    attention_out = attend(queries, keys_cache, values_cache, new_keys, new_values, cache_lengths)
    return (moe_out, attention_out)
```

```python
import functools
import jax
import jax.numpy as jnp
from jax import lax
from jax.experimental import pallas as pl
from jax.experimental.pallas import tpu as pltpu
from jax.sharding import PartitionSpec as P

EPS = 1e-06
LANES = 128


def pack_kernel(hidden_ref, gain_ref, ids_ref, gates_ref, packed_ref):
    rows, width = hidden_ref.shape
    lanes = packed_ref.shape[1] - width
    hidden = hidden_ref[...].astype(jnp.float32)
    scale = lax.rsqrt(jnp.mean(hidden * hidden, axis=-1, keepdims=True) + EPS)
    packed_ref[:, :width] = (hidden * scale * gain_ref[...].astype(jnp.float32)).astype(jnp.bfloat16)
    expert = lax.broadcasted_iota(jnp.int32, (lanes, rows), 0)
    weight = jnp.zeros((lanes, rows), jnp.float32)
    for k in range(ids_ref.shape[0]):
        gate = gates_ref[k : k + 1, :].astype(jnp.float32)
        weight = weight + jnp.where(ids_ref[k : k + 1, :] == expert, gate, 0.0)
    row = lax.broadcasted_iota(jnp.int32, (rows, rows), 0)
    column = lax.broadcasted_iota(jnp.int32, (rows, rows), 1)
    packed_ref[:, width:] = lax.dot_general(
        (row == column).astype(jnp.bfloat16),
        weight.astype(jnp.bfloat16),
        (((1,), (1,)), ((), ())),
        preferred_element_type=jnp.float32,
    ).astype(jnp.bfloat16)


def pack(moe_input, norm_gain, route_ids, route_gates, experts):
    rows, width = moe_input.shape
    lanes = -(-experts // LANES) * LANES
    return pl.pallas_call(
        pack_kernel,
        out_shape=jax.ShapeDtypeStruct((rows, width + lanes), jnp.bfloat16),
        name="pack",
        compiler_params=pltpu.CompilerParams(vmem_limit_bytes=2 << 20),
        cost_estimate=pl.CostEstimate(flops=rows * width * 8, bytes_accessed=rows * width * 4, transcendentals=rows),
    )(moe_input, norm_gain.reshape(1, width), route_ids.T, route_gates.T)


def expert_kernel(first_ref, second_ref, gate_ref, up_ref, down_ref, kept_ref, sent_ref, total_ref):
    step = pl.program_id(0)
    width = gate_ref.shape[1]
    half = first_ref.shape[0]
    rows = jnp.concatenate([first_ref[:, :width], second_ref[:, :width]], axis=0)
    gate_part = jnp.dot(rows, gate_ref[0], preferred_element_type=jnp.float32)
    up_part = jnp.dot(rows, up_ref[0], preferred_element_type=jnp.float32)
    active = (gate_part / (1.0 + jnp.exp(-gate_part)) * up_part).astype(jnp.bfloat16)
    part = jnp.dot(active, down_ref[0], preferred_element_type=jnp.float32)

    @pl.when(step == 0)
    def _():
        total_ref[...] = part

    @pl.when(step > 0)
    def _():
        total_ref[...] += part

    @pl.when(step == pl.num_programs(0) - 1)
    def _():
        expert = lax.axis_index("req")
        for source, target, base in ((first_ref, kept_ref, 0), (second_ref, sent_ref, half)):
            weights = source[:, width:].astype(jnp.float32)
            mine = lax.broadcasted_iota(jnp.int32, weights.shape, 1) == expert
            weight = jnp.sum(jnp.where(mine, weights, 0.0), axis=1, keepdims=True)
            produced = total_ref[base : base + half, :].astype(jnp.bfloat16).astype(jnp.float32)
            target[...] = (produced * weight).astype(target.dtype)


def expert_section(first, second, w_gate, w_up, w_down):
    half, packed = first.shape
    _, width, hidden = w_gate.shape
    tile = 256 if hidden % 256 == 0 else hidden
    steps = hidden // tile
    return pl.pallas_call(
        expert_kernel,
        grid=(steps,),
        in_specs=[
            pl.BlockSpec((half, packed), lambda j: (0, 0)),
            pl.BlockSpec((half, packed), lambda j: (0, 0)),
            pl.BlockSpec((1, width, tile), lambda j: (0, 0, j)),
            pl.BlockSpec((1, width, tile), lambda j: (0, 0, j)),
            pl.BlockSpec((1, tile, width), lambda j: (0, j, 0)),
        ],
        out_specs=[
            pl.BlockSpec((half, width), lambda j: (0, 0)),
            pl.BlockSpec((half, width), lambda j: (0, 0)),
        ],
        out_shape=[
            jax.ShapeDtypeStruct((half, width), jnp.float32),
            jax.ShapeDtypeStruct((half, width), jnp.bfloat16),
        ],
        scratch_shapes=[pltpu.VMEM((2 * half, width), jnp.float32)],
        name="experts",
        compiler_params=pltpu.CompilerParams(vmem_limit_bytes=32 << 20),
        cost_estimate=pl.CostEstimate(
            flops=12 * half * width * hidden,
            bytes_accessed=6 * width * hidden + 8 * half * width,
            transcendentals=2 * half * hidden,
        ),
    )(first, second, w_gate, w_up, w_down)


def exchange(value, distance, devices):
    return lax.ppermute(value, "req", [(i, i ^ distance) for i in range(devices)])


def gathered_layer(packed, w_gate, w_up, w_down, hidden, devices):
    rows, width = hidden.shape
    far = range(4, devices, 4)
    column = jnp.concatenate([packed] + [exchange(packed, k, devices) for k in far], axis=0)
    plane = jnp.concatenate([column, exchange(column, 2, devices)], axis=0)
    other = exchange(plane, 1, devices)
    kept, sent = expert_section(plane, other, w_gate, w_up, w_down)
    kept = kept + exchange(sent, 1, devices).astype(jnp.float32)
    half = kept.shape[0] // 2
    kept = kept[:half] + exchange(kept[half:].astype(jnp.bfloat16), 2, devices).astype(jnp.float32)
    total = hidden.astype(jnp.float32) + kept[:rows]
    for i, k in enumerate(far):
        block = kept[(i + 1) * rows : (i + 2) * rows].astype(jnp.bfloat16)
        total = total + exchange(block, k, devices).astype(jnp.float32)
    return total.astype(jnp.bfloat16)


def slot_table(route_ids, experts, capacity):
    onehot = (route_ids[:, :, None] == jnp.arange(experts, dtype=jnp.int32)[None, None, :]).astype(
        jnp.float32
    )
    present = jnp.sum(onehot, axis=1)
    earlier = jnp.cumsum(present, axis=0) - present
    levels = jnp.arange(capacity, dtype=jnp.float32)
    placed = present[:, :, None] * (earlier[:, :, None] == levels[None, None, :]).astype(
        jnp.float32
    )
    return (onehot, placed)


def expert_apply(received, w_gate, w_up, w_down):
    gate_part = jnp.einsum("nesd,edf->nesf", received, w_gate, preferred_element_type=jnp.float32)
    up_part = jnp.einsum("nesd,edf->nesf", received, w_up, preferred_element_type=jnp.float32)
    active = (jax.nn.silu(gate_part) * up_part).astype(jnp.bfloat16)
    return jnp.einsum("nesf,efd->nesd", active, w_down, preferred_element_type=jnp.float32).astype(
        jnp.bfloat16
    )


def attend(queries, keys_cache, values_cache, new_keys, new_values, cache_lengths):
    batch_rows = queries.shape[0]
    kv_heads = keys_cache.shape[1]
    cache_span = keys_cache.shape[2]
    head_size = keys_cache.shape[3]
    group_heads = queries.shape[1] // (kv_heads * head_size)
    score_scale = head_size ** (-0.5)
    grouped = queries.reshape(batch_rows, kv_heads, group_heads, head_size)
    scores = (
        jnp.einsum("bgqd,bgld->bgql", grouped, keys_cache, preferred_element_type=jnp.float32)
        * score_scale
    )
    own_score = (
        jnp.einsum(
            "bgqd,bgd->bgq",
            grouped,
            new_keys.reshape(batch_rows, kv_heads, head_size),
            preferred_element_type=jnp.float32,
        )
        * score_scale
    )
    live_mask = (jnp.arange(cache_span, dtype=jnp.int32)[None, :] < cache_lengths[:, None])[
        :, None, None, :
    ]
    highest = jnp.maximum(jnp.max(jnp.where(live_mask, scores, -jnp.inf), axis=-1), own_score)
    weights = jnp.where(live_mask, jnp.exp(scores - highest[..., None]), 0.0)
    own_weight = jnp.exp(own_score - highest)
    totals = jnp.sum(weights, axis=-1) + own_weight
    prob_low = (weights / totals[..., None]).astype(jnp.bfloat16)
    own_prob = (own_weight / totals).astype(jnp.bfloat16)
    mixed_out = jnp.einsum(
        "bgql,bgld->bgqd", prob_low, values_cache, preferred_element_type=jnp.float32
    )
    mixed_out = mixed_out + own_prob.astype(jnp.float32)[..., None] * new_values.reshape(
        batch_rows, kv_heads, 1, head_size
    ).astype(jnp.float32)
    return mixed_out.reshape(batch_rows, -1).astype(jnp.bfloat16)


def slotted_layer(
    moe_input, norm_gain, route_ids, route_gates, expert_gate, expert_up, expert_down, capacity
):
    row_count = moe_input.shape[0]
    model_width = moe_input.shape[1]
    local_experts = expert_gate.shape[0]
    devices = lax.axis_size("req")
    experts = devices * local_experts
    hidden = moe_input.astype(jnp.float32)
    normed = (
        hidden
        * lax.rsqrt(jnp.mean(hidden * hidden, axis=-1, keepdims=True) + EPS)
        * norm_gain.astype(jnp.float32)
    ).astype(jnp.bfloat16)
    onehot, placed = slot_table(route_ids, experts, capacity)
    selector = placed.reshape(row_count, experts * capacity).astype(jnp.bfloat16)
    outgoing = jnp.einsum("rs,rd->sd", selector, normed, preferred_element_type=jnp.float32).astype(
        jnp.bfloat16
    )
    outgoing = outgoing.reshape(devices, local_experts, capacity, model_width)
    produced = expert_apply(
        lax.all_to_all(outgoing, "req", split_axis=0, concat_axis=0, tiled=True),
        expert_gate,
        expert_up,
        expert_down,
    )
    returned = lax.all_to_all(produced, "req", split_axis=0, concat_axis=0, tiled=True)
    weight = jnp.einsum("rke,rk->re", onehot, route_gates.astype(jnp.float32))
    combine = (
        (weight[:, :, None] * placed).reshape(row_count, experts * capacity).astype(jnp.bfloat16)
    )
    expert_sum = jnp.dot(
        combine,
        returned.reshape(experts * capacity, model_width),
        preferred_element_type=jnp.float32,
    )
    moe_out = (hidden + expert_sum).astype(jnp.bfloat16)
    return moe_out


def body(
    moe_input,
    norm_gain,
    route_ids,
    route_gates,
    expert_gate,
    expert_up,
    expert_down,
    queries,
    keys_cache,
    values_cache,
    new_keys,
    new_values,
    cache_lengths,
):
    row_count = moe_input.shape[0]
    model_width = moe_input.shape[1]
    local_experts = expert_gate.shape[0]
    devices = lax.axis_size("req")
    experts = devices * local_experts
    capacity = min(row_count, max(2, 16 * row_count // experts))
    if local_experts == 1 and capacity == row_count and devices >= 8 and devices & (devices - 1) == 0:
        packed = pack(moe_input, norm_gain, route_ids, route_gates, experts)
        moe_out = gathered_layer(packed, expert_gate, expert_up, expert_down, moe_input, devices)
    else:
        moe_out = slotted_layer(
            moe_input, norm_gain, route_ids, route_gates, expert_gate, expert_up, expert_down, capacity
        )
    attention_out = attend(queries, keys_cache, values_cache, new_keys, new_values, cache_lengths)
    return (moe_out, attention_out)


def solution(mesh):
    in_specs = (
        P(("grp", "req"), None),
        P(),
        P(("grp", "req"), None),
        P(("grp", "req"), None),
        P("req", None, None),
        P("req", None, None),
        P("req", None, None),
        P(("grp", "req"), None),
        P(("grp", "req"), None, None, None),
        P(("grp", "req"), None, None, None),
        P(("grp", "req"), None),
        P(("grp", "req"), None),
        P(("grp", "req")),
    )
    out_specs = (P(("grp", "req"), None), P(("grp", "req"), None))
    return jax.shard_map(body, mesh=mesh, in_specs=in_specs, out_specs=out_specs, check_vma=False)
```

```python
import functools
import jax
import jax.numpy as jnp
from jax import lax
from jax.experimental import pallas as pl
from jax.experimental.pallas import tpu as pltpu
from jax.sharding import PartitionSpec as P


EPS = 1e-06
LANES = 128
ANY = pl.BlockSpec(memory_space=pl.ANY)
VMEM = pl.BlockSpec(memory_space=pltpu.VMEM)


def in_hbm(array):
    return pltpu.with_memory_space_constraint(array, pltpu.HBM)


def pack_kernel(hidden_hbm, gain_hbm, ids_hbm, gates_hbm, packed_ref, hidden_ref, gain_ref, ids_ref, gates_ref, sems):
    copies = [
        pltpu.make_async_copy(source, target, sems.at[i])
        for i, (source, target) in enumerate(
            ((hidden_hbm, hidden_ref), (gain_hbm, gain_ref), (ids_hbm, ids_ref), (gates_hbm, gates_ref))
        )
    ]
    for copy in copies:
        copy.start()
    for copy in copies:
        copy.wait()
    rows, width = hidden_ref.shape
    lanes = packed_ref.shape[1] - width
    hidden = hidden_ref[...].astype(jnp.float32)
    scale = lax.rsqrt(jnp.mean(hidden * hidden, axis=-1, keepdims=True) + EPS)
    for j in range(width // LANES):
        span = slice(j * LANES, (j + 1) * LANES)
        gain = gain_ref[j : j + 1, :].astype(jnp.float32)
        packed_ref[:, span] = (hidden[:, span] * scale * gain).astype(jnp.bfloat16)
    expert = lax.broadcasted_iota(jnp.int32, (lanes, rows), 0)
    weight = jnp.zeros((lanes, rows), jnp.float32)
    for k in range(ids_ref.shape[0]):
        gate = gates_ref[k : k + 1, :].astype(jnp.float32)
        weight = weight + jnp.where(ids_ref[k : k + 1, :] == expert, gate, 0.0)
    row = lax.broadcasted_iota(jnp.int32, (rows, rows), 0)
    column = lax.broadcasted_iota(jnp.int32, (rows, rows), 1)
    packed_ref[:, width:] = lax.dot_general(
        (row == column).astype(jnp.bfloat16),
        weight.astype(jnp.bfloat16),
        (((1,), (1,)), ((), ())),
        preferred_element_type=jnp.float32,
    ).astype(jnp.bfloat16)


def pack(moe_input, norm_gain, route_ids, route_gates, experts):
    rows, width = moe_input.shape
    lanes = -(-experts // LANES) * LANES
    operands = (moe_input, norm_gain.reshape(width // LANES, LANES), route_ids.T, route_gates.T)
    return pl.pallas_call(
        pack_kernel,
        in_specs=[ANY] * 4,
        out_specs=VMEM,
        out_shape=pltpu.VMEM((rows, width + lanes), jnp.bfloat16),
        scratch_shapes=[pltpu.VMEM(a.shape, a.dtype) for a in operands] + [pltpu.SemaphoreType.DMA((4,))],
        name="pack",
        compiler_params=pltpu.CompilerParams(vmem_limit_bytes=2 << 20),
        cost_estimate=pl.CostEstimate(flops=rows * width * 8, bytes_accessed=rows * width * 4, transcendentals=rows),
    )(*map(in_hbm, operands))


def load_kernel(pieces, count, *refs):
    sources, targets, sems = refs[:count], refs[-1 - count : -1], refs[-1]
    copies = []
    for i, (source, target) in enumerate(zip(sources, targets)):
        size = source.shape[1] // pieces
        for j in range(pieces):
            span = pl.ds(j * size, size)
            copies.append(
                pltpu.make_async_copy(source.at[0, span, :], target.at[span, :], sems.at[i * pieces + j])
            )
    for copy in copies:
        copy.start()
    for copy in copies:
        copy.wait()


def load_weights(weights, after):
    pieces = 4
    count = len(weights)
    size = sum(w.size for w in weights)
    return pl.pallas_call(
        functools.partial(load_kernel, pieces, count),
        in_specs=[ANY] * (count + len(after)),
        out_specs=[VMEM] * count,
        out_shape=[pltpu.VMEM(w.shape[1:], w.dtype) for w in weights],
        scratch_shapes=[pltpu.SemaphoreType.DMA((pieces * count,))],
        name="load",
        compiler_params=pltpu.CompilerParams(vmem_limit_bytes=1 << 20),
        cost_estimate=pl.CostEstimate(flops=200 * size, bytes_accessed=2 * size, transcendentals=0),
    )(*map(in_hbm, weights), *after)


def expert_kernel(first_ref, second_ref, gate_ref, up_ref, down_ref, kept_ref, sent_ref, active_ref):
    width, hidden = gate_ref.shape
    half = first_ref.shape[0]
    tile = 256 if hidden % 256 == 0 else hidden
    rows = jnp.concatenate([first_ref[:, :width], second_ref[:, :width]], axis=0)
    for j in range(0, hidden, tile):
        gate_part = jnp.dot(rows, gate_ref[:, j : j + tile], preferred_element_type=jnp.float32)
        up_part = jnp.dot(rows, up_ref[:, j : j + tile], preferred_element_type=jnp.float32)
        active = gate_part / (1.0 + jnp.exp(-gate_part)) * up_part
        active_ref[:, j : j + tile] = active.astype(jnp.bfloat16)
    expert = lax.axis_index("req")
    packed = jnp.concatenate([first_ref[:, width:], second_ref[:, width:]], axis=0).astype(jnp.float32)
    mine = lax.broadcasted_iota(jnp.int32, packed.shape, 1) == expert
    weight = jnp.sum(jnp.where(mine, packed, 0.0), axis=1, keepdims=True)
    tile = 512 if width % 512 == 0 else width
    for j in range(0, width, tile):
        produced = jnp.dot(active_ref[...], down_ref[:, j : j + tile], preferred_element_type=jnp.float32)
        produced = produced.astype(jnp.bfloat16).astype(jnp.float32) * weight
        kept_ref[:, j : j + tile] = produced[:half]
        sent_ref[:, j : j + tile] = produced[half:].astype(jnp.bfloat16)


def expert_section(first, second, w_gate, w_up, w_down):
    half, _ = first.shape
    width, hidden = w_gate.shape
    return pl.pallas_call(
        expert_kernel,
        in_specs=[VMEM] * 5,
        out_specs=[VMEM] * 2,
        out_shape=[
            pltpu.VMEM((half, width), jnp.float32),
            pltpu.VMEM((half, width), jnp.bfloat16),
        ],
        scratch_shapes=[pltpu.VMEM((2 * half, hidden), jnp.bfloat16)],
        name="experts",
        compiler_params=pltpu.CompilerParams(vmem_limit_bytes=8 << 20),
        cost_estimate=pl.CostEstimate(
            flops=12 * half * width * hidden,
            bytes_accessed=6 * width * hidden + 8 * half * width,
            transcendentals=2 * half * hidden,
        ),
    )(first, second, w_gate, w_up, w_down)


def attend_kernel(queries_hbm, keys_hbm, values_hbm, new_keys_hbm, new_values_hbm, lengths_ref, out_ref,
                  queries_ref, keys_ref, values_ref, new_keys_ref, new_values_ref, small_sems, sems):
    batch, heads, span, size = keys_ref.shape
    group = queries_ref.shape[1] // (heads * size)
    small = [
        pltpu.make_async_copy(source, target, small_sems.at[i])
        for i, (source, target) in enumerate(
            ((queries_hbm, queries_ref), (new_keys_hbm, new_keys_ref), (new_values_hbm, new_values_ref))
        )
    ]
    large = []
    for b in range(batch):
        large.append(pltpu.make_async_copy(keys_hbm.at[b], keys_ref.at[b], sems.at[2 * b]))
        large.append(pltpu.make_async_copy(values_hbm.at[b], values_ref.at[b], sems.at[2 * b + 1]))
    for copy in small + large:
        copy.start()
    for copy in small:
        copy.wait()
    queries = queries_ref[...].astype(jnp.float32)
    new_keys = new_keys_ref[...].astype(jnp.float32)
    new_values = new_values_ref[...].astype(jnp.float32)
    position = lax.broadcasted_iota(jnp.int32, (group, span), 1)
    for b in range(batch):
        large[2 * b].wait()
        live = position < lengths_ref[b]
        probs = []
        for h in range(heads):
            first = h * group
            query = jnp.concatenate(
                [queries[b : b + 1, (first + i) * size : (first + i + 1) * size] for i in range(group)], axis=0
            )
            scores = lax.dot_general(
                query.astype(jnp.bfloat16),
                keys_ref[b, h],
                (((1,), (1,)), ((), ())),
                preferred_element_type=jnp.float32,
            ) * (size ** -0.5)
            own = jnp.sum(query * new_keys[b : b + 1, h * size : (h + 1) * size], axis=1, keepdims=True)
            own = own * (size ** -0.5)
            highest = jnp.maximum(jnp.max(jnp.where(live, scores, -jnp.inf), axis=1, keepdims=True), own)
            weights = jnp.where(live, jnp.exp(scores - highest), 0.0)
            own_weight = jnp.exp(own - highest)
            totals = jnp.sum(weights, axis=1, keepdims=True) + own_weight
            probs.append(((weights / totals).astype(jnp.bfloat16), (own_weight / totals).astype(jnp.bfloat16)))
        large[2 * b + 1].wait()
        for h, (prob, own_prob) in enumerate(probs):
            mixed = jnp.dot(prob, values_ref[b, h], preferred_element_type=jnp.float32)
            mixed = mixed + own_prob.astype(jnp.float32) * new_values[b : b + 1, h * size : (h + 1) * size]
            mixed = mixed.astype(out_ref.dtype)
            for i in range(group):
                column = (h * group + i) * size
                out_ref[b : b + 1, column : column + size] = mixed[i : i + 1]


def attend(queries, keys_cache, values_cache, new_keys, new_values, cache_lengths):
    operands = (queries, keys_cache, values_cache, new_keys, new_values)
    batch, _, span, size = keys_cache.shape
    return pl.pallas_call(
        attend_kernel,
        in_specs=[ANY] * 5 + [pl.BlockSpec(memory_space=pltpu.SMEM)],
        out_specs=VMEM,
        out_shape=jax.ShapeDtypeStruct(queries.shape, queries.dtype),
        scratch_shapes=[pltpu.VMEM(a.shape, a.dtype) for a in operands]
        + [pltpu.SemaphoreType.DMA((3,)), pltpu.SemaphoreType.DMA((2 * batch,))],
        name="attend",
        compiler_params=pltpu.CompilerParams(vmem_limit_bytes=12 << 20),
        cost_estimate=pl.CostEstimate(
            flops=200 * keys_cache.size, bytes_accessed=4 * keys_cache.size, transcendentals=queries.size * span // size
        ),
    )(*map(in_hbm, operands), cache_lengths)


def exchange(value, distance, devices):
    return lax.ppermute(value, "req", [(i, i ^ distance) for i in range(devices)])


def gathered_layer(packed, w_gate, w_up, w_down, hidden, devices):
    rows, _ = hidden.shape
    far = range(4, devices, 4)
    column = jnp.concatenate([packed] + [exchange(packed, k, devices) for k in far], axis=0)
    weights = load_weights((w_gate, w_up, w_down), ())
    plane = jnp.concatenate([column, exchange(column, 2, devices)], axis=0)
    other = exchange(plane, 1, devices)
    kept, sent = expert_section(plane, other, *weights)
    kept = kept + exchange(sent, 1, devices).astype(jnp.float32)
    half = kept.shape[0] // 2
    kept = kept[:half] + exchange(kept[half:].astype(jnp.bfloat16), 2, devices).astype(jnp.float32)
    total = hidden.astype(jnp.float32) + kept[:rows]
    for i, k in enumerate(far):
        block = kept[(i + 1) * rows : (i + 2) * rows].astype(jnp.bfloat16)
        total = total + exchange(block, k, devices).astype(jnp.float32)
    return total.astype(jnp.bfloat16)


def slot_table(route_ids, experts, capacity):
    onehot = (route_ids[:, :, None] == jnp.arange(experts, dtype=jnp.int32)[None, None, :]).astype(
        jnp.float32
    )
    present = jnp.sum(onehot, axis=1)
    earlier = jnp.cumsum(present, axis=0) - present
    levels = jnp.arange(capacity, dtype=jnp.float32)
    placed = present[:, :, None] * (earlier[:, :, None] == levels[None, None, :]).astype(
        jnp.float32
    )
    return (onehot, placed)


def expert_apply(received, w_gate, w_up, w_down):
    gate_part = jnp.einsum("nesd,edf->nesf", received, w_gate, preferred_element_type=jnp.float32)
    up_part = jnp.einsum("nesd,edf->nesf", received, w_up, preferred_element_type=jnp.float32)
    active = (jax.nn.silu(gate_part) * up_part).astype(jnp.bfloat16)
    return jnp.einsum("nesf,efd->nesd", active, w_down, preferred_element_type=jnp.float32).astype(
        jnp.bfloat16
    )


def slotted_layer(
    moe_input, norm_gain, route_ids, route_gates, expert_gate, expert_up, expert_down, capacity
):
    row_count = moe_input.shape[0]
    model_width = moe_input.shape[1]
    local_experts = expert_gate.shape[0]
    devices = lax.axis_size("req")
    experts = devices * local_experts
    hidden = moe_input.astype(jnp.float32)
    normed = (
        hidden
        * lax.rsqrt(jnp.mean(hidden * hidden, axis=-1, keepdims=True) + EPS)
        * norm_gain.astype(jnp.float32)
    ).astype(jnp.bfloat16)
    onehot, placed = slot_table(route_ids, experts, capacity)
    selector = placed.reshape(row_count, experts * capacity).astype(jnp.bfloat16)
    outgoing = jnp.einsum("rs,rd->sd", selector, normed, preferred_element_type=jnp.float32).astype(
        jnp.bfloat16
    )
    outgoing = outgoing.reshape(devices, local_experts, capacity, model_width)
    produced = expert_apply(
        lax.all_to_all(outgoing, "req", split_axis=0, concat_axis=0, tiled=True),
        expert_gate,
        expert_up,
        expert_down,
    )
    returned = lax.all_to_all(produced, "req", split_axis=0, concat_axis=0, tiled=True)
    weight = jnp.einsum("rke,rk->re", onehot, route_gates.astype(jnp.float32))
    combine = (
        (weight[:, :, None] * placed).reshape(row_count, experts * capacity).astype(jnp.bfloat16)
    )
    expert_sum = jnp.dot(
        combine,
        returned.reshape(experts * capacity, model_width),
        preferred_element_type=jnp.float32,
    )
    moe_out = (hidden + expert_sum).astype(jnp.bfloat16)
    return moe_out


def layer(
    moe_input,
    norm_gain,
    route_ids,
    route_gates,
    expert_gate,
    expert_up,
    expert_down,
    queries,
    keys_cache,
    values_cache,
    new_keys,
    new_values,
    cache_lengths,
):
    row_count = moe_input.shape[0]
    local_experts = expert_gate.shape[0]
    devices = lax.axis_size("req")
    experts = devices * local_experts
    capacity = min(row_count, max(2, 16 * row_count // experts))
    if local_experts == 1 and capacity == row_count and devices >= 8 and devices & (devices - 1) == 0:
        packed = pack(moe_input, norm_gain, route_ids, route_gates, experts)
        moe_out = gathered_layer(packed, expert_gate, expert_up, expert_down, moe_input, devices)
    else:
        moe_out = slotted_layer(
            moe_input, norm_gain, route_ids, route_gates, expert_gate, expert_up, expert_down, capacity
        )
    attention_out = attend(queries, keys_cache, values_cache, new_keys, new_values, cache_lengths)
    return (moe_out, attention_out)


def solution(mesh):
    in_specs = (
        P(("grp", "req"), None),
        P(),
        P(("grp", "req"), None),
        P(("grp", "req"), None),
        P("req", None, None),
        P("req", None, None),
        P("req", None, None),
        P(("grp", "req"), None),
        P(("grp", "req"), None, None, None),
        P(("grp", "req"), None, None, None),
        P(("grp", "req"), None),
        P(("grp", "req"), None),
        P(("grp", "req")),
    )
    out_specs = (P(("grp", "req"), None), P(("grp", "req"), None))
    return jax.shard_map(layer, mesh=mesh, in_specs=in_specs, out_specs=out_specs, check_vma=False)
```
